256 devices in a mesh: row: 16 (over z, core), col: 16 (over y, x).
Axes of the slice: x: 4, y: 4, z: 8, core: 2. Of those that a mesh axis runs over, the one named last changes fastest.
Arguments:
- matrix: float32 [12288, 12288], P('row', 'col'), may hold values from -8 to 8
Outputs:
- updated: float32 [12288, 12288], P('row', 'col')
- reflectors: float32 [16, 12288], replicated
- coefficients: float32 [2, 16], replicated
The draws below stay inside these ranges and needn't reach their ends.
All inputs are finite; a program needn't handle non-finite values.
Results may differ from the reference program's by a relative error of at most 0.0003.
Values sent between devices are 32-bit elements; how exact they have to be, the bound alone decides.
No kernel may reach another device: no remote copies, remote signals or barrier semaphores. Data moves between devices by JAX's collectives and lax.ppermute only.
A program may use at most 64 MiB of HBM per device.

```python
import jax
import jax.numpy as jnp
from jax import lax

ORDER = 12288
PANEL_COLUMNS = 16


def draw_matrix(key, part):
    first = jax.random.fold_in(jax.random.fold_in(key, 11), 0)
    raw = jax.random.normal(first, (ORDER, ORDER), jnp.float32)
    sym = (raw + raw.T) * jnp.float32(0.7071067811865476)
    return jnp.clip(sym, -8.0, 8.0)


def setup_inputs(seed: int = 0) -> dict:
    splits = jax.random.split(jax.random.key(seed), 2)
    return {
        "matrix": draw_matrix(jax.random.fold_in(splits[1], 71), 0),
    }


HIGH = lax.Precision.HIGHEST

def reference(matrix):
    order = matrix.shape[0]
    positions = jnp.arange(order, dtype=jnp.int32)
    reflectors = jnp.zeros((PANEL_COLUMNS, order), jnp.float32)
    reflected_images = jnp.zeros((PANEL_COLUMNS, order), jnp.float32)
    reflector_scales = []
    below_diagonal = []
    for step in range(PANEL_COLUMNS):
        column = matrix[:, step] - jnp.dot(reflected_images[:, step], reflectors, precision=HIGH) - jnp.dot(reflectors[:, step], reflected_images, precision=HIGH)
        below = jnp.where(positions > step, column, 0.0)
        leading = column[step + 1]
        norm_value = jnp.sqrt(jnp.sum(below * below))
        reflector = jnp.where(positions == step + 1, 1.0, below / (leading + norm_value))
        reflector_scale = 1.0 + leading / norm_value
        product = jnp.dot(matrix, reflector, precision=HIGH)
        images_dot = jnp.dot(reflected_images, reflector, precision=HIGH)
        reflect_dot = jnp.dot(reflectors, reflector, precision=HIGH)
        image = reflector_scale * (product - jnp.dot(images_dot, reflectors, precision=HIGH) - jnp.dot(reflect_dot, reflected_images, precision=HIGH))
        image = image - 0.5 * reflector_scale * jnp.sum(image * reflector) * reflector
        reflectors = reflectors.at[step].set(reflector)
        reflected_images = reflected_images.at[step].set(image)
        reflector_scales.append(reflector_scale)
        below_diagonal.append(-norm_value)
    left_side = jnp.concatenate([reflectors, reflected_images], axis=0)
    right_side = jnp.concatenate([reflected_images, reflectors], axis=0)
    updated = matrix - jnp.einsum('kr,kc->rc', left_side, right_side, precision=HIGH)
    coefficients = jnp.stack([jnp.stack(reflector_scales), jnp.stack(below_diagonal)])
    return (updated, reflectors, coefficients)
```

```python
import jax
import jax.numpy as jnp
from jax import lax
from jax.experimental import pallas as pl
from jax.experimental.pallas import tpu as pltpu
from jax.sharding import PartitionSpec as P

PANEL_COLUMNS = 16
LANES = 128
TILES = 12
SCALE, COEF = TILES, TILES + 1
OWN = 48

VMEM = pl.BlockSpec(memory_space=pltpu.VMEM)
SMEM = pl.BlockSpec(memory_space=pltpu.SMEM)
ANY = pl.BlockSpec(memory_space=pl.ANY)


def total(x):
    return jnp.sum(jnp.sum(x, axis=0, keepdims=True), axis=1, keepdims=True)


def iota(shape, dim):
    return lax.broadcasted_iota(jnp.int32, shape, dim)


def unpack(load):
    lane = iota((8, LANES), 1)
    tiles = []
    for gm in range(4):
        q = [load(8 * gm + k) for k in range(8)]
        tiles.append(jnp.where(lane < 48, q[0], jnp.where(lane < 96, q[1], q[2])))
        tiles.append(jnp.where(lane < 16, q[2], jnp.where(lane < 64, q[3], jnp.where(lane < 112, q[4], q[5]))))
        tiles.append(jnp.where(lane < 32, q[5], jnp.where(lane < 80, q[6], q[7])))
    return tiles


def tree_sum(xs):
    xs = list(xs)
    while len(xs) > 1:
        xs = [xs[i] + xs[i + 1] if i + 1 < len(xs) else xs[i] for i in range(0, len(xs), 2)]
    return xs[0]


def position(m):
    return (iota((8, LANES), 0) * TILES + m) * LANES + iota((8, LANES), 1)


def message(first, second, offset):
    row, lane = iota((OWN, LANES), 0), iota((OWN, LANES), 1)
    here = (row + offset) & (LANES - 1)
    there = (row + offset + OWN) & (LANES - 1)
    picked = jnp.where(lane == here, first, 0.0) + jnp.where(lane == there, second, 0.0)
    return jnp.sum(picked, axis=0, keepdims=True)


def own_column(rows_ref, k):
    head = rows_ref[0, :, 0:LANES]
    return jnp.sum(jnp.where(iota((OWN, LANES), 1) == k, head, 0.0), axis=1, keepdims=True)


def first_body(own, rows_ref, out_ref):
    out_ref[...] = jnp.broadcast_to(
        message(own_column(rows_ref, 0), own_column(rows_ref, 1), own[0]), out_ref.shape
    )


def image_of(got_ref, h_ref, u, scale):
    y = unpack(lambda first: got_ref[pl.ds(first, 8, stride=32), :])
    p = [scale * (y[m] - h_ref[m]) for m in range(TILES)]
    kappa = 0.5 * scale * total(tree_sum(p[m] * u[m] for m in range(TILES)))
    return p, kappa


def step_body(col, own, got_ref, base_ref, h_ref, u_ref, rows_ref, w_ref, un_ref, out_ref, flat_ref):
    j = col[0]
    u = [u_ref[m] for m in range(TILES)]
    scale = u_ref[SCALE, 0:1, 0:1]
    p, kappa = image_of(got_ref, h_ref, u, scale)
    lane1 = iota((1, LANES), 1)

    def at(x, k):
        return jnp.sum(jnp.where(lane1 == k, x[0:1, :], 0.0), axis=1, keepdims=True)

    factor = at(p[0], j) - kappa * at(u[0], j) - kappa
    leading = at(base_ref[0], j + 1) - at(p[0], j + 1) - factor * at(u[0], j + 1)
    below = []
    for m in range(TILES):
        column = base_ref[m] - p[m] - factor * u[m]
        if m == 0:
            column = jnp.where(position(m) > j, column, 0.0)
        below.append(column)
        rest = jnp.where(position(m) == j + 1, 0.0, column) if m == 0 else column
        flat_ref[pl.ds(m, 8, stride=TILES), :] = rest
    norm = jnp.sqrt(total(tree_sum(b * b for b in below)))
    inverse = 1.0 / (leading + norm)
    scale_now = 1.0 + leading / norm
    acc = [jnp.zeros((OWN, LANES), jnp.float32) for _ in range(2)]
    for s in range(96):
        k, t = divmod(s, 6)
        acc[s % 2] = acc[s % 2] + rows_ref[k, :, LANES * t : LANES * (t + 1)] * flat_ref[s : s + 1, :]
    product = jnp.sum(acc[0] + acc[1], axis=1, keepdims=True) * inverse + own_column(rows_ref, j + 1)
    out_ref[...] = jnp.broadcast_to(
        message(product, own_column(rows_ref, j + 2), own[0]), out_ref.shape
    )
    for m in range(TILES):
        w_ref[m] = p[m] - kappa * u[m]
        r = below[m] * inverse
        un_ref[m] = jnp.where(position(m) == j + 1, 1.0, r) if m == 0 else r
    un_ref[SCALE] = jnp.broadcast_to(scale_now, (8, LANES))
    lane8, row8 = iota((8, LANES), 1), iota((8, LANES), 0)
    un_ref[COEF] = jnp.where(lane8 == j, jnp.where(row8 == 0, scale_now, -norm), u_ref[COEF])


def history_body(col, got_ref, w_ref, u_ref, un_ref, hist_ref, base_ref, h_ref, hist_out, hist, sems):
    j = col[0]
    row = (j + PANEL_COLUMNS - 1) % PANEL_COLUMNS
    whole = pltpu.make_async_copy(hist_ref, hist, sems.at[0])
    whole.start()
    lane1 = iota((1, LANES), 1)
    h = [jnp.zeros((8, LANES), jnp.float32) for _ in range(TILES)]
    base = unpack(lambda first: pltpu.roll(got_ref[pl.ds(first, 8, stride=32), :], LANES - OWN, 1))
    un = [un_ref[m] for m in range(TILES)]
    whole.wait()
    keep_v = pltpu.make_async_copy(u_ref.at[pl.ds(0, TILES)], hist_out.at[0, row], sems.at[1])
    keep_w = pltpu.make_async_copy(w_ref, hist_out.at[1, row], sems.at[2])
    keep_v.start()
    keep_w.start()
    for m in range(TILES):
        hist[0, row, m] = u_ref[m]
        hist[1, row, m] = w_ref[m]
    for i in range(PANEL_COLUMNS):
        v = [hist[0, i, m] for m in range(TILES)]
        w = [hist[1, i, m] for m in range(TILES)]
        vu = total(tree_sum(v[m] * un[m] for m in range(TILES)))
        wu = total(tree_sum(w[m] * un[m] for m in range(TILES)))
        vj = jnp.sum(jnp.where(lane1 == j + 1, v[0][0:1, :], 0.0), axis=1, keepdims=True)
        wj = jnp.sum(jnp.where(lane1 == j + 1, w[0][0:1, :], 0.0), axis=1, keepdims=True)
        for m in range(TILES):
            h[m] = h[m] + (wu * v[m] + vu * w[m])
            base[m] = base[m] - (wj * v[m] + vj * w[m])
    for m in range(TILES):
        h_ref[m] = h[m]
        base_ref[m] = base[m]
    keep_v.wait()
    keep_w.wait()


def last_body(own, got_ref, h_ref, u_ref, hist_ref, matrix_ref, updated_ref, whole_ref, hist, block, whole, sides, sems):
    read_hist = pltpu.make_async_copy(hist_ref, hist, sems.at[0])
    read_block = pltpu.make_async_copy(matrix_ref, block, sems.at[1])
    read_hist.start()
    read_block.start()
    u = [u_ref[m] for m in range(TILES)]
    p, kappa = image_of(got_ref, h_ref, u, u_ref[SCALE, 0:1, 0:1])
    read_hist.wait()
    per = TILES * 8
    for m in range(TILES):
        n = (PANEL_COLUMNS - 1) * per + 8 * m
        hist[0, n : n + 8, :] = u[m]
        hist[1, n : n + 8, :] = p[m] - kappa * u[m]
    for side, n in ((0, own[1]), (1, own[2])):
        z, m0 = n // 2, 6 * (n % 2)
        for t in range(6):
            for half in range(2):
                rows = pl.ds(half * 8 * per + 8 * (m0 + t) + z, 8, stride=per)
                for k in range(2):
                    at = 16 * k + 8 * half
                    sides[side, at : at + 8, LANES * t : LANES * (t + 1)] = hist[k ^ side, rows, :]

    def pieces(x):
        high = x.astype(jnp.bfloat16)
        rest = x - high.astype(jnp.float32)
        mid = rest.astype(jnp.bfloat16)
        return high, mid, (rest - mid.astype(jnp.float32)).astype(jnp.bfloat16)

    lh, lm, ll = pieces(sides[0].T)
    rh, rm, rl = pieces(sides[1])
    left = jnp.concatenate([lh, lh, lm, lm, lh, ll], axis=1)
    right = jnp.concatenate([rh, rm, rh, rm, rl, rh], axis=0)
    read_block.wait()
    writes = []
    step = 256
    for n in range(block.shape[0] // step):
        rows = slice(step * n, step * (n + 1))
        block[rows, :] = block[rows, :] - jnp.dot(left[rows, :], right, preferred_element_type=jnp.float32)
        writes.append(pltpu.make_async_copy(block.at[rows, :], updated_ref.at[rows, :], sems.at[2 + n]))
        writes[-1].start()
    for half in range(2):
        for m in range(TILES):
            for z in range(8):
                s = TILES * z + m
                rows = pl.ds(half * 8 * per + 8 * m + z, 8, stride=per)
                whole[8 * half : 8 * half + 8, LANES * s : LANES * (s + 1)] = hist[0, rows, :]
    write = pltpu.make_async_copy(whole, whole_ref, sems.at[5])
    write.start()
    for w in writes:
        w.wait()
    write.wait()


def per_device(matrix):
    f32 = jnp.float32
    r, c = lax.axis_index("row"), lax.axis_index("col")
    ways = lax.axis_size("col")
    devices = ways * lax.axis_size("row")
    tile_cols = matrix.shape[1]
    own = jnp.stack([(OWN * (r * ways + c)) & (LANES - 1), r, c])
    rows = lax.all_to_all(
        matrix.reshape(ways, OWN, tile_cols), "col", split_axis=0, concat_axis=0, tiled=True
    )

    def exchange(packed):
        return lax.all_to_all(packed, ("row", "col"), split_axis=0, concat_axis=0, tiled=True)

    def shape(*dims):
        return jax.ShapeDtypeStruct(dims, f32)

    vec, ext, packed = shape(TILES, 8, LANES), shape(TILES + 2, 8, LANES), shape(devices, LANES)
    hist = shape(2, PANEL_COLUMNS, TILES, 8, LANES)
    order = TILES * 8 * LANES
    first = pl.pallas_call(first_body, out_shape=packed, in_specs=[SMEM, VMEM], out_specs=VMEM, name="first")
    step = pl.pallas_call(
        step_body,
        out_shape=(vec, ext, packed),
        in_specs=[SMEM] * 2 + [VMEM] * 5,
        out_specs=(VMEM,) * 3,
        scratch_shapes=[pltpu.VMEM((order // LANES, LANES), f32)],
        name="step",
    )
    history = pl.pallas_call(
        history_body,
        out_shape=(vec, vec, hist),
        in_specs=[SMEM] + [VMEM] * 4 + [ANY],
        out_specs=(VMEM, VMEM, ANY),
        input_output_aliases={5: 2},
        scratch_shapes=[pltpu.VMEM(hist.shape, f32), pltpu.SemaphoreType.DMA((3,))],
        name="history",
    )
    last = pl.pallas_call(
        last_body,
        out_shape=(shape(*matrix.shape), shape(PANEL_COLUMNS, order)),
        in_specs=[SMEM] + [VMEM] * 3 + [ANY] * 2,
        out_specs=(ANY, ANY),
        scratch_shapes=[
            pltpu.VMEM((2, PANEL_COLUMNS * TILES * 8, LANES), f32),
            pltpu.VMEM(matrix.shape, f32),
            pltpu.VMEM((PANEL_COLUMNS, order), f32),
            pltpu.VMEM((2, 2 * PANEL_COLUMNS, tile_cols), f32),
            pltpu.SemaphoreType.DMA((6,)),
        ],
        name="last",
    )

    def one_column(j, state):
        got, base, h, u, kept = state
        col = jnp.reshape(j, (1,))
        w, un, out = step(col, own, got, base, h, u, rows)
        got_next = exchange(out)
        base, h, kept = history(col, got, w, u, un, kept)
        return got_next, base, h, un, kept

    def zeros(s):
        return jnp.zeros(s.shape, f32)

    u = jnp.concatenate([zeros(vec), jnp.full((1, 8, LANES), -1.0, f32), jnp.zeros((1, 8, LANES), f32)])
    state = (exchange(first(own, rows)), zeros(vec), zeros(vec), u, zeros(hist))
    got, _, h, u, kept = lax.fori_loop(0, PANEL_COLUMNS, one_column, state)
    updated, whole = last(own, got, h, u, kept.reshape(2, -1, LANES), matrix)
    return updated, whole, u[COEF, :2, :PANEL_COLUMNS]


def solution(mesh):
    return jax.shard_map(
        per_device,
        mesh=mesh,
        in_specs=(P("row", "col"),),
        out_specs=(P("row", "col"), P(), P()),
        check_vma=False,
    )
```

```python
import jax
import jax.numpy as jnp
from jax import lax
from jax.experimental import pallas as pl
from jax.experimental.pallas import tpu as pltpu
from jax.sharding import PartitionSpec as P

PANEL_COLUMNS = 16
LANES = 128
TILES = 12
SCALE, COEF = TILES, TILES + 1
OWN = 48

VMEM = pl.BlockSpec(memory_space=pltpu.VMEM)
SMEM = pl.BlockSpec(memory_space=pltpu.SMEM)
ANY = pl.BlockSpec(memory_space=pl.ANY)


def total(x):
    return jnp.sum(jnp.sum(x, axis=0, keepdims=True), axis=1, keepdims=True)


def iota(shape, dim):
    return lax.broadcasted_iota(jnp.int32, shape, dim)


def unpack(load):
    lane = iota((8, LANES), 1)
    tiles = []
    for gm in range(4):
        q = [load(8 * gm + k) for k in range(8)]
        tiles.append(jnp.where(lane < 48, q[0], jnp.where(lane < 96, q[1], q[2])))
        tiles.append(jnp.where(lane < 16, q[2], jnp.where(lane < 64, q[3], jnp.where(lane < 112, q[4], q[5]))))
        tiles.append(jnp.where(lane < 32, q[5], jnp.where(lane < 80, q[6], q[7])))
    return tiles


def tree_sum(xs):
    xs = list(xs)
    while len(xs) > 1:
        xs = [xs[i] + xs[i + 1] if i + 1 < len(xs) else xs[i] for i in range(0, len(xs), 2)]
    return xs[0]


def position(m):
    return (iota((8, LANES), 0) * TILES + m) * LANES + iota((8, LANES), 1)


def message(first, second, slots_ref):
    return jnp.sum(slots_ref[0] * first + slots_ref[1] * second, axis=0, keepdims=True)


def own_column(rows_ref, k):
    head = rows_ref[0, :, 0:LANES]
    return jnp.sum(jnp.where(iota((OWN, LANES), 1) == k, head, 0.0), axis=1, keepdims=True)


def begin_body(top_ref, out_ref, tmp):
    lane = iota((8, LANES), 1)
    for t in range(6):
        tmp[32 * t : 32 * (t + 1), :] = top_ref[:, LANES * t : LANES * (t + 1)]

    def tile(k, m):
        half, t = divmod(m, 6)
        return tmp[pl.ds(32 * t + 2 * half + k, 8, stride=4), :]

    for gm in range(4):
        rows = []
        for k in range(2):
            t = [tile(k, 3 * gm + n) for n in range(3)]
            rows.append([t[0], t[0], jnp.where(lane < 96, t[1], t[0]), t[1], t[1], jnp.where(lane < 112, t[2], t[1]), t[2], t[2]])
        for q in range(8):
            mine = ((lane - OWN * q) & (LANES - 1)) < OWN
            out_ref[pl.ds(8 * gm + q, 8, stride=32), :] = jnp.where(mine, rows[0][q], pltpu.roll(rows[1][q], OWN, 1))


def image_of(got_ref, h_ref, u, scale):
    y = unpack(lambda first: got_ref[pl.ds(first, 8, stride=32), :])
    p = [scale * (y[m] - h_ref[m]) for m in range(TILES)]
    kappa = 0.5 * scale * total(tree_sum(p[m] * u[m] for m in range(TILES)))
    return p, kappa


def step_body(col, slots_ref, got_ref, base_ref, h_ref, u_ref, rows_ref, w_ref, un_ref, out_ref, flat_ref):
    j = col[0]
    u = [u_ref[m] for m in range(TILES)]
    scale = u_ref[SCALE, 0:1, 0:1]
    p, kappa = image_of(got_ref, h_ref, u, scale)
    lane1 = iota((1, LANES), 1)

    def at(x, k):
        return jnp.sum(jnp.where(lane1 == k, x[0:1, :], 0.0), axis=1, keepdims=True)

    factor = at(p[0], j) - kappa * at(u[0], j) - kappa
    leading = at(base_ref[0], j + 1) - at(p[0], j + 1) - factor * at(u[0], j + 1)
    below = []
    for m in range(TILES):
        column = base_ref[m] - p[m] - factor * u[m]
        if m == 0:
            column = jnp.where(position(m) > j, column, 0.0)
        below.append(column)
        rest = jnp.where(position(m) == j + 1, 0.0, column) if m == 0 else column
        flat_ref[pl.ds(m, 8, stride=TILES), :] = rest
    norm = jnp.sqrt(total(tree_sum(b * b for b in below)))
    inverse = 1.0 / (leading + norm)
    scale_now = 1.0 + leading / norm
    acc = [jnp.zeros((OWN, LANES), jnp.float32) for _ in range(2)]
    for s in range(96):
        k, t = divmod(s, 6)
        acc[s % 2] = acc[s % 2] + rows_ref[k, :, LANES * t : LANES * (t + 1)] * flat_ref[s : s + 1, :]
    product = jnp.sum(acc[0] + acc[1], axis=1, keepdims=True) * inverse + own_column(rows_ref, j + 1)
    out_ref[...] = jnp.broadcast_to(
        message(product, own_column(rows_ref, j + 2), slots_ref), out_ref.shape
    )
    for m in range(TILES):
        w_ref[m] = p[m] - kappa * u[m]
        r = below[m] * inverse
        un_ref[m] = jnp.where(position(m) == j + 1, 1.0, r) if m == 0 else r
    un_ref[SCALE] = jnp.broadcast_to(scale_now, (8, LANES))
    lane8, row8 = iota((8, LANES), 1), iota((8, LANES), 0)
    un_ref[COEF] = jnp.where(lane8 == j, jnp.where(row8 == 0, scale_now, -norm), u_ref[COEF])


def history_body(col, got_ref, w_ref, u_ref, un_ref, hist_ref, base_ref, h_ref, hist_out, hist, sems):
    j = col[0]
    row = (j + PANEL_COLUMNS - 1) % PANEL_COLUMNS
    whole = pltpu.make_async_copy(hist_ref, hist, sems.at[0])
    whole.start()
    lane1 = iota((1, LANES), 1)
    h = [jnp.zeros((8, LANES), jnp.float32) for _ in range(TILES)]
    base = unpack(lambda first: pltpu.roll(got_ref[pl.ds(first, 8, stride=32), :], LANES - OWN, 1))
    un = [un_ref[m] for m in range(TILES)]
    whole.wait()
    keep_v = pltpu.make_async_copy(u_ref.at[pl.ds(0, TILES)], hist_out.at[0, row], sems.at[1])
    keep_w = pltpu.make_async_copy(w_ref, hist_out.at[1, row], sems.at[2])
    keep_v.start()
    keep_w.start()
    for m in range(TILES):
        hist[0, row, m] = u_ref[m]
        hist[1, row, m] = w_ref[m]
    for i in range(PANEL_COLUMNS):
        v = [hist[0, i, m] for m in range(TILES)]
        w = [hist[1, i, m] for m in range(TILES)]
        vu = total(tree_sum(v[m] * un[m] for m in range(TILES)))
        wu = total(tree_sum(w[m] * un[m] for m in range(TILES)))
        vj = jnp.sum(jnp.where(lane1 == j + 1, v[0][0:1, :], 0.0), axis=1, keepdims=True)
        wj = jnp.sum(jnp.where(lane1 == j + 1, w[0][0:1, :], 0.0), axis=1, keepdims=True)
        for m in range(TILES):
            h[m] = h[m] + (wu * v[m] + vu * w[m])
            base[m] = base[m] - (wj * v[m] + vj * w[m])
    for m in range(TILES):
        h_ref[m] = h[m]
        base_ref[m] = base[m]
    keep_v.wait()
    keep_w.wait()


def last_body(own, got_ref, h_ref, u_ref, hist_ref, matrix_ref, updated_ref, whole_ref, hist, block, whole, sides, sems):
    read_hist = pltpu.make_async_copy(hist_ref, hist, sems.at[0])
    read_block = pltpu.make_async_copy(matrix_ref, block, sems.at[1])
    read_hist.start()
    read_block.start()
    u = [u_ref[m] for m in range(TILES)]
    p, kappa = image_of(got_ref, h_ref, u, u_ref[SCALE, 0:1, 0:1])
    read_hist.wait()
    per = TILES * 8
    for m in range(TILES):
        n = (PANEL_COLUMNS - 1) * per + 8 * m
        hist[0, n : n + 8, :] = u[m]
        hist[1, n : n + 8, :] = p[m] - kappa * u[m]
    for side, n in ((0, own[0]), (1, own[1])):
        z, m0 = n // 2, 6 * (n % 2)
        for t in range(6):
            for half in range(2):
                rows = pl.ds(half * 8 * per + 8 * (m0 + t) + z, 8, stride=per)
                for k in range(2):
                    at = 16 * k + 8 * half
                    sides[side, at : at + 8, LANES * t : LANES * (t + 1)] = hist[k ^ side, rows, :]

    def pieces(x):
        high = x.astype(jnp.bfloat16)
        rest = x - high.astype(jnp.float32)
        mid = rest.astype(jnp.bfloat16)
        return high, mid, (rest - mid.astype(jnp.float32)).astype(jnp.bfloat16)

    lh, lm, ll = pieces(sides[0].T)
    rh, rm, rl = pieces(sides[1])
    left = jnp.concatenate([lh, lh, lm, lm, lh, ll], axis=1)
    right = jnp.concatenate([rh, rm, rh, rm, rl, rh], axis=0)
    read_block.wait()
    writes = []
    step = 256
    for n in range(block.shape[0] // step):
        rows = slice(step * n, step * (n + 1))
        block[rows, :] = block[rows, :] - jnp.dot(left[rows, :], right, preferred_element_type=jnp.float32)
        writes.append(pltpu.make_async_copy(block.at[rows, :], updated_ref.at[rows, :], sems.at[2 + n]))
        writes[-1].start()
    for half in range(2):
        for m in range(TILES):
            for z in range(8):
                s = TILES * z + m
                rows = pl.ds(half * 8 * per + 8 * m + z, 8, stride=per)
                whole[8 * half : 8 * half + 8, LANES * s : LANES * (s + 1)] = hist[0, rows, :]
    write = pltpu.make_async_copy(whole, whole_ref, sems.at[5])
    write.start()
    for w in writes:
        w.wait()
    write.wait()


def per_device(matrix):
    f32 = jnp.float32
    r, c = lax.axis_index("row"), lax.axis_index("col")
    ways = lax.axis_size("col")
    devices = ways * lax.axis_size("row")
    tile_cols = matrix.shape[1]
    own = jnp.stack([r, c])
    rows = lax.all_to_all(
        matrix.reshape(ways, OWN, tile_cols), "col", split_axis=0, concat_axis=0, tiled=True
    )
    top = jnp.where(r == 0, matrix[:2], 0.0)
    for far in (8, 4, 2, 1):
        top = top + lax.ppermute(top, "row", [(n, n + far) for n in range(0, 16, 2 * far)])
    for bit in (1, 2, 4, 8):
        other = lax.ppermute(top, "col", [(n, n ^ bit) for n in range(ways)])
        low = (c & bit) == 0
        top = jnp.concatenate([jnp.where(low, top, other), jnp.where(low, other, top)])
    place = iota((2, OWN, LANES), 2) - iota((2, OWN, LANES), 1) - OWN * (r * ways + c + iota((2, OWN, LANES), 0))
    slots = jnp.where((place & (LANES - 1)) == 0, 1.0, 0.0).astype(f32)

    def exchange(packed):
        return lax.all_to_all(packed, ("row", "col"), split_axis=0, concat_axis=0, tiled=True)

    def shape(*dims):
        return jax.ShapeDtypeStruct(dims, f32)

    vec, ext, packed = shape(TILES, 8, LANES), shape(TILES + 2, 8, LANES), shape(devices, LANES)
    hist = shape(2, PANEL_COLUMNS, TILES, 8, LANES)
    order = TILES * 8 * LANES
    begin = pl.pallas_call(begin_body, out_shape=packed, in_specs=[VMEM], out_specs=VMEM, scratch_shapes=[pltpu.VMEM((192, LANES), f32)], name="begin")
    step = pl.pallas_call(
        step_body,
        out_shape=(vec, ext, packed),
        in_specs=[SMEM] + [VMEM] * 6,
        out_specs=(VMEM,) * 3,
        scratch_shapes=[pltpu.VMEM((order // LANES, LANES), f32)],
        name="step",
    )
    history = pl.pallas_call(
        history_body,
        out_shape=(vec, vec, hist),
        in_specs=[SMEM] + [VMEM] * 4 + [ANY],
        out_specs=(VMEM, VMEM, ANY),
        input_output_aliases={5: 2},
        scratch_shapes=[pltpu.VMEM(hist.shape, f32), pltpu.SemaphoreType.DMA((3,))],
        name="history",
    )
    last = pl.pallas_call(
        last_body,
        out_shape=(shape(*matrix.shape), shape(PANEL_COLUMNS, order)),
        in_specs=[SMEM] + [VMEM] * 3 + [ANY] * 2,
        out_specs=(ANY, ANY),
        scratch_shapes=[
            pltpu.VMEM((2, PANEL_COLUMNS * TILES * 8, LANES), f32),
            pltpu.VMEM(matrix.shape, f32),
            pltpu.VMEM((PANEL_COLUMNS, order), f32),
            pltpu.VMEM((2, 2 * PANEL_COLUMNS, tile_cols), f32),
            pltpu.SemaphoreType.DMA((6,)),
        ],
        name="last",
    )

    def one_column(j, state):
        got, base, h, u, kept = state
        col = jnp.reshape(j, (1,))
        w, un, out = step(col, slots, got, base, h, u, rows)
        got_next = exchange(out)
        base, h, kept = history(col, got, w, u, un, kept)
        return got_next, base, h, un, kept

    def zeros(s):
        return jnp.zeros(s.shape, f32)

    u = jnp.concatenate([zeros(vec), jnp.full((1, 8, LANES), -1.0, f32), jnp.zeros((1, 8, LANES), f32)])
    state = (begin(top), zeros(vec), zeros(vec), u, zeros(hist))
    got, _, h, u, kept = lax.fori_loop(0, PANEL_COLUMNS, one_column, state)
    updated, whole = last(own, got, h, u, kept.reshape(2, -1, LANES), matrix)
    return updated, whole, u[COEF, :2, :PANEL_COLUMNS]


def solution(mesh):
    return jax.shard_map(
        per_device,
        mesh=mesh,
        in_specs=(P("row", "col"),),
        out_specs=(P("row", "col"), P(), P()),
        check_vma=False,
    )
```

```python
import jax
import jax.numpy as jnp
from jax import lax
from jax.experimental import pallas as pl
from jax.experimental.pallas import tpu as pltpu
from jax.sharding import PartitionSpec as P

PANEL_COLUMNS = 16
LANES = 128
TILES = 12
SCALE, COEF = TILES, TILES + 1
OWN = 48

VMEM = pl.BlockSpec(memory_space=pltpu.VMEM)
SMEM = pl.BlockSpec(memory_space=pltpu.SMEM)
ANY = pl.BlockSpec(memory_space=pl.ANY)


def total(x):
    return jnp.sum(jnp.sum(x, axis=0, keepdims=True), axis=1, keepdims=True)


def iota(shape, dim):
    return lax.broadcasted_iota(jnp.int32, shape, dim)


def unpack(load):
    lane = iota((8, LANES), 1)
    tiles = []
    for gm in range(4):
        q = [load(8 * gm + k) for k in range(8)]
        tiles.append(jnp.where(lane < 48, q[0], jnp.where(lane < 96, q[1], q[2])))
        tiles.append(jnp.where(lane < 16, q[2], jnp.where(lane < 64, q[3], jnp.where(lane < 112, q[4], q[5]))))
        tiles.append(jnp.where(lane < 32, q[5], jnp.where(lane < 80, q[6], q[7])))
    return tiles


def tree_sum(xs):
    xs = list(xs)
    while len(xs) > 1:
        xs = [xs[i] + xs[i + 1] if i + 1 < len(xs) else xs[i] for i in range(0, len(xs), 2)]
    return xs[0]


def position(m):
    return (iota((8, LANES), 0) * TILES + m) * LANES + iota((8, LANES), 1)


def message(first, second):
    device = lax.axis_index("row") * lax.axis_size("col") + lax.axis_index("col")
    place = iota((OWN, LANES), 1) - iota((OWN, LANES), 0) - OWN * device
    picked = jnp.where((place & (LANES - 1)) == 0, first, 0.0) + jnp.where((place & (LANES - 1)) == OWN, second, 0.0)
    return jnp.sum(picked, axis=0, keepdims=True)


def own_column(rows_ref, k):
    head = rows_ref[0, :, 0:LANES]
    return jnp.sum(jnp.where(iota((OWN, LANES), 1) == k, head, 0.0), axis=1, keepdims=True)


def begin_body(top_ref, out_ref, hist_ref, tmp, zero, sem):
    zero[...] = jnp.zeros(zero.shape, jnp.float32)
    clear = [pltpu.make_async_copy(zero, hist_ref.at[n], sem.at[n]) for n in range(2)]
    for copy in clear:
        copy.start()
    lane = iota((8, LANES), 1)
    for t in range(6):
        tmp[32 * t : 32 * (t + 1), :] = top_ref[:, LANES * t : LANES * (t + 1)]

    def tile(k, m):
        half, t = divmod(m, 6)
        return tmp[pl.ds(32 * t + 2 * half + k, 8, stride=4), :]

    for gm in range(4):
        rows = []
        for k in range(2):
            t = [tile(k, 3 * gm + n) for n in range(3)]
            rows.append([t[0], t[0], jnp.where(lane < 96, t[1], t[0]), t[1], t[1], jnp.where(lane < 112, t[2], t[1]), t[2], t[2]])
        for q in range(8):
            mine = ((lane - OWN * q) & (LANES - 1)) < OWN
            out_ref[pl.ds(8 * gm + q, 8, stride=32), :] = jnp.where(mine, rows[0][q], pltpu.roll(rows[1][q], OWN, 1))
    for copy in clear:
        copy.wait()


def image_of(got_ref, h_ref, u, scale):
    y = unpack(lambda first: got_ref[pl.ds(first, 8, stride=32), :])
    p = [scale * (y[m] - h_ref[m]) for m in range(TILES)]
    kappa = 0.5 * scale * total(tree_sum(p[m] * u[m] for m in range(TILES)))
    return p, kappa


def step_body(col, got_ref, base_ref, h_ref, u_ref, rows_ref, w_ref, un_ref, out_ref, flat_ref):
    j = col[0]
    u = [u_ref[m] for m in range(TILES)]
    scale = u_ref[SCALE, 0:1, 0:1]
    p, kappa = image_of(got_ref, h_ref, u, scale)
    lane1 = iota((1, LANES), 1)

    def at(x, k):
        return jnp.sum(jnp.where(lane1 == k, x[0:1, :], 0.0), axis=1, keepdims=True)

    factor = at(p[0], j) - kappa * at(u[0], j) - kappa
    leading = at(base_ref[0], j + 1) - at(p[0], j + 1) - factor * at(u[0], j + 1)
    below = []
    for m in range(TILES):
        column = base_ref[m] - p[m] - factor * u[m]
        if m == 0:
            column = jnp.where(position(m) > j, column, 0.0)
        below.append(column)
        rest = jnp.where(position(m) == j + 1, 0.0, column) if m == 0 else column
        flat_ref[pl.ds(m, 8, stride=TILES), :] = rest
    norm = jnp.sqrt(total(tree_sum(b * b for b in below)))
    inverse = 1.0 / (leading + norm)
    scale_now = 1.0 + leading / norm
    acc = [jnp.zeros((OWN, LANES), jnp.float32) for _ in range(2)]
    for s in range(96):
        k, t = divmod(s, 6)
        acc[s % 2] = acc[s % 2] + rows_ref[k, :, LANES * t : LANES * (t + 1)] * flat_ref[s : s + 1, :]
    product = jnp.sum(acc[0] + acc[1], axis=1, keepdims=True) * inverse + own_column(rows_ref, j + 1)
    out_ref[...] = jnp.broadcast_to(
        message(product, own_column(rows_ref, j + 2)), out_ref.shape
    )
    for m in range(TILES):
        w_ref[m] = p[m] - kappa * u[m]
        r = below[m] * inverse
        un_ref[m] = jnp.where(position(m) == j + 1, 1.0, r) if m == 0 else r
    un_ref[SCALE] = jnp.broadcast_to(scale_now, (8, LANES))
    lane8, row8 = iota((8, LANES), 1), iota((8, LANES), 0)
    un_ref[COEF] = jnp.where(lane8 == j, jnp.where(row8 == 0, scale_now, -norm), u_ref[COEF])


def history_body(col, got_ref, w_ref, u_ref, un_ref, hist_ref, base_ref, h_ref, hist_out, hist, sems):
    j = col[0]
    row = (j + PANEL_COLUMNS - 1) % PANEL_COLUMNS
    whole = pltpu.make_async_copy(hist_ref, hist, sems.at[0])
    whole.start()
    lane1 = iota((1, LANES), 1)
    h = [jnp.zeros((8, LANES), jnp.float32) for _ in range(TILES)]
    base = unpack(lambda first: pltpu.roll(got_ref[pl.ds(first, 8, stride=32), :], LANES - OWN, 1))
    un = [un_ref[m] for m in range(TILES)]
    whole.wait()
    keep_v = pltpu.make_async_copy(u_ref.at[pl.ds(0, TILES)], hist_out.at[0, row], sems.at[1])
    keep_w = pltpu.make_async_copy(w_ref, hist_out.at[1, row], sems.at[2])
    keep_v.start()
    keep_w.start()
    for m in range(TILES):
        hist[0, row, m] = u_ref[m]
        hist[1, row, m] = w_ref[m]
    for i in range(PANEL_COLUMNS):
        v = [hist[0, i, m] for m in range(TILES)]
        w = [hist[1, i, m] for m in range(TILES)]
        vu = total(tree_sum(v[m] * un[m] for m in range(TILES)))
        wu = total(tree_sum(w[m] * un[m] for m in range(TILES)))
        vj = jnp.sum(jnp.where(lane1 == j + 1, v[0][0:1, :], 0.0), axis=1, keepdims=True)
        wj = jnp.sum(jnp.where(lane1 == j + 1, w[0][0:1, :], 0.0), axis=1, keepdims=True)
        for m in range(TILES):
            h[m] = h[m] + (wu * v[m] + vu * w[m])
            base[m] = base[m] - (wj * v[m] + vj * w[m])
    for m in range(TILES):
        h_ref[m] = h[m]
        base_ref[m] = base[m]
    keep_v.wait()
    keep_w.wait()


def last_body(own, got_ref, h_ref, u_ref, hist_ref, matrix_ref, updated_ref, whole_ref, hist, block, whole, sides, sems):
    read_hist = pltpu.make_async_copy(hist_ref, hist, sems.at[0])
    read_block = pltpu.make_async_copy(matrix_ref, block, sems.at[1])
    read_hist.start()
    read_block.start()
    u = [u_ref[m] for m in range(TILES)]
    p, kappa = image_of(got_ref, h_ref, u, u_ref[SCALE, 0:1, 0:1])
    read_hist.wait()
    per = TILES * 8
    for m in range(TILES):
        n = (PANEL_COLUMNS - 1) * per + 8 * m
        hist[0, n : n + 8, :] = u[m]
        hist[1, n : n + 8, :] = p[m] - kappa * u[m]
    for side, n in ((0, own[0]), (1, own[1])):
        z, m0 = n // 2, 6 * (n % 2)
        for t in range(6):
            for half in range(2):
                rows = pl.ds(half * 8 * per + 8 * (m0 + t) + z, 8, stride=per)
                for k in range(2):
                    at = 16 * k + 8 * half
                    sides[side, at : at + 8, LANES * t : LANES * (t + 1)] = hist[k ^ side, rows, :]

    def pieces(x):
        high = x.astype(jnp.bfloat16)
        rest = x - high.astype(jnp.float32)
        mid = rest.astype(jnp.bfloat16)
        return high, mid, (rest - mid.astype(jnp.float32)).astype(jnp.bfloat16)

    lh, lm, ll = pieces(sides[0].T)
    rh, rm, rl = pieces(sides[1])
    left = jnp.concatenate([lh, lh, lm, lm, lh, ll], axis=1)
    right = jnp.concatenate([rh, rm, rh, rm, rl, rh], axis=0)
    read_block.wait()
    writes = []
    step = 256
    for n in range(block.shape[0] // step):
        rows = slice(step * n, step * (n + 1))
        block[rows, :] = block[rows, :] - jnp.dot(left[rows, :], right, preferred_element_type=jnp.float32)
        writes.append(pltpu.make_async_copy(block.at[rows, :], updated_ref.at[rows, :], sems.at[2 + n]))
        writes[-1].start()
    for half in range(2):
        for m in range(TILES):
            for z in range(8):
                s = TILES * z + m
                rows = pl.ds(half * 8 * per + 8 * m + z, 8, stride=per)
                whole[8 * half : 8 * half + 8, LANES * s : LANES * (s + 1)] = hist[0, rows, :]
    write = pltpu.make_async_copy(whole, whole_ref, sems.at[5])
    write.start()
    for w in writes:
        w.wait()
    write.wait()


def per_device(matrix):
    f32 = jnp.float32
    r, c = lax.axis_index("row"), lax.axis_index("col")
    ways = lax.axis_size("col")
    devices = ways * lax.axis_size("row")
    tile_cols = matrix.shape[1]
    own = jnp.stack([r, c])
    top = lax.all_to_all(
        jnp.broadcast_to(matrix[:2], (ways, 2, tile_cols)), "col", split_axis=0, concat_axis=0, tiled=True
    ).reshape(2 * ways, tile_cols)
    top, matrix_after = lax.optimization_barrier((top, matrix))
    top = jnp.where(r == 0, top, 0.0)
    for far in (8, 4, 2, 1):
        top = top + lax.ppermute(top, "row", [(n, n + far) for n in range(0, 16, 2 * far)])
    rows = lax.all_to_all(
        matrix_after.reshape(ways, OWN, tile_cols), "col", split_axis=0, concat_axis=0, tiled=True
    )

    def exchange(packed):
        return lax.all_to_all(packed, ("row", "col"), split_axis=0, concat_axis=0, tiled=True)

    def shape(*dims):
        return jax.ShapeDtypeStruct(dims, f32)

    vec, ext, packed = shape(TILES, 8, LANES), shape(TILES + 2, 8, LANES), shape(devices, LANES)
    hist = shape(2, PANEL_COLUMNS, TILES, 8, LANES)
    order = TILES * 8 * LANES
    begin = pl.pallas_call(
        begin_body,
        out_shape=(packed, hist),
        in_specs=[VMEM],
        out_specs=(VMEM, ANY),
        scratch_shapes=[
            pltpu.VMEM((192, LANES), f32),
            pltpu.VMEM(hist.shape[1:], f32),
            pltpu.SemaphoreType.DMA((2,)),
        ],
        name="begin",
    )
    step = pl.pallas_call(
        step_body,
        out_shape=(vec, ext, packed),
        in_specs=[SMEM] + [VMEM] * 5,
        out_specs=(VMEM,) * 3,
        scratch_shapes=[pltpu.VMEM((order // LANES, LANES), f32)],
        name="step",
    )
    history = pl.pallas_call(
        history_body,
        out_shape=(vec, vec, hist),
        in_specs=[SMEM] + [VMEM] * 4 + [ANY],
        out_specs=(VMEM, VMEM, ANY),
        input_output_aliases={5: 2},
        scratch_shapes=[pltpu.VMEM(hist.shape, f32), pltpu.SemaphoreType.DMA((3,))],
        name="history",
    )
    last = pl.pallas_call(
        last_body,
        out_shape=(shape(*matrix.shape), shape(PANEL_COLUMNS, order)),
        in_specs=[SMEM] + [VMEM] * 3 + [ANY] * 2,
        out_specs=(ANY, ANY),
        scratch_shapes=[
            pltpu.VMEM((2, PANEL_COLUMNS * TILES * 8, LANES), f32),
            pltpu.VMEM(matrix.shape, f32),
            pltpu.VMEM((PANEL_COLUMNS, order), f32),
            pltpu.VMEM((2, 2 * PANEL_COLUMNS, tile_cols), f32),
            pltpu.SemaphoreType.DMA((6,)),
        ],
        name="last",
    )

    def one_column(j, state):
        got, base, h, u, kept = state
        col = jnp.reshape(j, (1,))
        w, un, out = step(col, got, base, h, u, rows)
        got_next = exchange(out)
        base, h, kept = history(col, got, w, u, un, kept)
        return got_next, base, h, un, kept

    def zeros(s):
        return jnp.zeros(s.shape, f32)

    u = jnp.concatenate([zeros(vec), jnp.full((1, 8, LANES), -1.0, f32), jnp.zeros((1, 8, LANES), f32)])
    got, kept = begin(top)
    state = (got, zeros(vec), zeros(vec), u, kept)
    got, _, h, u, kept = lax.fori_loop(0, PANEL_COLUMNS, one_column, state)
    updated, whole = last(own, got, h, u, kept.reshape(2, -1, LANES), matrix)
    return updated, whole, u[COEF, :2, :PANEL_COLUMNS]


def solution(mesh):
    return jax.shard_map(
        per_device,
        mesh=mesh,
        in_specs=(P("row", "col"),),
        out_specs=(P("row", "col"), P(), P()),
        check_vma=False,
    )
```

```python
import jax
import jax.numpy as jnp
from jax import lax
from jax.experimental import pallas as pl
from jax.experimental.pallas import tpu as pltpu
from jax.sharding import PartitionSpec as P

PANEL_COLUMNS = 16
LANES = 128
TILES = 12
SCALE, COEF = TILES, TILES + 1
OWN = 48

VMEM = pl.BlockSpec(memory_space=pltpu.VMEM)
SMEM = pl.BlockSpec(memory_space=pltpu.SMEM)
ANY = pl.BlockSpec(memory_space=pl.ANY)


def total(x):
    return jnp.sum(jnp.sum(x, axis=0, keepdims=True), axis=1, keepdims=True)


def iota(shape, dim):
    return lax.broadcasted_iota(jnp.int32, shape, dim)


def unpack(load):
    lane = iota((8, LANES), 1)
    tiles = []
    for gm in range(4):
        q = [load(8 * gm + k) for k in range(8)]
        tiles.append(jnp.where(lane < 48, q[0], jnp.where(lane < 96, q[1], q[2])))
        tiles.append(jnp.where(lane < 16, q[2], jnp.where(lane < 64, q[3], jnp.where(lane < 112, q[4], q[5]))))
        tiles.append(jnp.where(lane < 32, q[5], jnp.where(lane < 80, q[6], q[7])))
    return tiles


def tree_sum(xs):
    xs = list(xs)
    while len(xs) > 1:
        xs = [xs[i] + xs[i + 1] if i + 1 < len(xs) else xs[i] for i in range(0, len(xs), 2)]
    return xs[0]


def position(m):
    return (iota((8, LANES), 0) * TILES + m) * LANES + iota((8, LANES), 1)


def message(first, second):
    device = lax.axis_index("row") * lax.axis_size("col") + lax.axis_index("col")
    place = iota((OWN, LANES), 1) - iota((OWN, LANES), 0) - OWN * device
    picked = jnp.where((place & (LANES - 1)) == 0, first, 0.0) + jnp.where((place & (LANES - 1)) == OWN, second, 0.0)
    return jnp.sum(picked, axis=0, keepdims=True)


def own_column(rows_ref, k):
    head = rows_ref[0, :, 0:LANES]
    return jnp.sum(jnp.where(iota((OWN, LANES), 1) == k, head, 0.0), axis=1, keepdims=True)


def begin_body(top_ref, out_ref, hist_ref, tmp):
    del hist_ref
    lane = iota((8, LANES), 1)
    for t in range(6):
        tmp[32 * t : 32 * (t + 1), :] = top_ref[:, LANES * t : LANES * (t + 1)]

    def tile(k, m):
        half, t = divmod(m, 6)
        return tmp[pl.ds(32 * t + 2 * half + k, 8, stride=4), :]

    for gm in range(4):
        rows = []
        for k in range(2):
            t = [tile(k, 3 * gm + n) for n in range(3)]
            rows.append([t[0], t[0], jnp.where(lane < 96, t[1], t[0]), t[1], t[1], jnp.where(lane < 112, t[2], t[1]), t[2], t[2]])
        for q in range(8):
            mine = ((lane - OWN * q) & (LANES - 1)) < OWN
            out_ref[pl.ds(8 * gm + q, 8, stride=32), :] = jnp.where(mine, rows[0][q], pltpu.roll(rows[1][q], OWN, 1))

def image_of(got_ref, h_ref, u, scale):
    y = unpack(lambda first: got_ref[pl.ds(first, 8, stride=32), :])
    p = [scale * (y[m] - h_ref[m]) for m in range(TILES)]
    kappa = 0.5 * scale * total(tree_sum(p[m] * u[m] for m in range(TILES)))
    return p, kappa


def step_body(col, got_ref, base_ref, h_ref, u_ref, rows_ref, w_ref, un_ref, out_ref, flat_ref):
    j = col[0]
    u = [u_ref[m] for m in range(TILES)]
    scale = u_ref[SCALE, 0:1, 0:1]
    p, kappa = image_of(got_ref, h_ref, u, scale)
    lane1 = iota((1, LANES), 1)

    def at(x, k):
        return jnp.sum(jnp.where(lane1 == k, x[0:1, :], 0.0), axis=1, keepdims=True)

    factor = at(p[0], j) - kappa * at(u[0], j) - kappa
    leading = at(base_ref[0], j + 1) - at(p[0], j + 1) - factor * at(u[0], j + 1)
    below = []
    for m in range(TILES):
        column = base_ref[m] - p[m] - factor * u[m]
        if m == 0:
            column = jnp.where(position(m) > j, column, 0.0)
        below.append(column)
        rest = jnp.where(position(m) == j + 1, 0.0, column) if m == 0 else column
        flat_ref[pl.ds(m, 8, stride=TILES), :] = rest
    norm = jnp.sqrt(total(tree_sum(b * b for b in below)))
    inverse = 1.0 / (leading + norm)
    scale_now = 1.0 + leading / norm
    acc = [jnp.zeros((OWN, LANES), jnp.float32) for _ in range(2)]
    for s in range(96):
        k, t = divmod(s, 6)
        acc[s % 2] = acc[s % 2] + rows_ref[k, :, LANES * t : LANES * (t + 1)] * flat_ref[s : s + 1, :]
    product = jnp.sum(acc[0] + acc[1], axis=1, keepdims=True) * inverse + own_column(rows_ref, j + 1)
    out_ref[...] = jnp.broadcast_to(
        message(product, own_column(rows_ref, j + 2)), out_ref.shape
    )
    for m in range(TILES):
        w_ref[m] = p[m] - kappa * u[m]
        r = below[m] * inverse
        un_ref[m] = jnp.where(position(m) == j + 1, 1.0, r) if m == 0 else r
    un_ref[SCALE] = jnp.broadcast_to(scale_now, (8, LANES))
    lane8, row8 = iota((8, LANES), 1), iota((8, LANES), 0)
    un_ref[COEF] = jnp.where(lane8 == j, jnp.where(row8 == 0, scale_now, -norm), u_ref[COEF])


def history_body(col, got_ref, w_ref, u_ref, un_ref, hist_ref, base_ref, h_ref, hist_out, hist, sems):
    j = col[0]
    row = (j + PANEL_COLUMNS - 1) % PANEL_COLUMNS
    whole = pltpu.make_async_copy(hist_ref, hist, sems.at[0])
    whole.start()
    lane1 = iota((1, LANES), 1)
    h = [jnp.zeros((8, LANES), jnp.float32) for _ in range(TILES)]
    base = unpack(lambda first: pltpu.roll(got_ref[pl.ds(first, 8, stride=32), :], LANES - OWN, 1))
    un = [un_ref[m] for m in range(TILES)]
    whole.wait()
    keep_v = pltpu.make_async_copy(u_ref.at[pl.ds(0, TILES)], hist_out.at[0, row], sems.at[1])
    keep_w = pltpu.make_async_copy(w_ref, hist_out.at[1, row], sems.at[2])
    keep_v.start()
    keep_w.start()
    for m in range(TILES):
        hist[0, row, m] = u_ref[m]
        hist[1, row, m] = w_ref[m]
    for i in range(PANEL_COLUMNS):
        kept = i < j
        v = [jnp.where(kept, hist[0, i, m], 0.0) for m in range(TILES)]
        w = [jnp.where(kept, hist[1, i, m], 0.0) for m in range(TILES)]
        vu = total(tree_sum(v[m] * un[m] for m in range(TILES)))
        wu = total(tree_sum(w[m] * un[m] for m in range(TILES)))
        vj = jnp.sum(jnp.where(lane1 == j + 1, v[0][0:1, :], 0.0), axis=1, keepdims=True)
        wj = jnp.sum(jnp.where(lane1 == j + 1, w[0][0:1, :], 0.0), axis=1, keepdims=True)
        for m in range(TILES):
            h[m] = h[m] + (wu * v[m] + vu * w[m])
            base[m] = base[m] - (wj * v[m] + vj * w[m])
    for m in range(TILES):
        h_ref[m] = h[m]
        base_ref[m] = base[m]
    keep_v.wait()
    keep_w.wait()


def last_body(own, got_ref, h_ref, u_ref, hist_ref, matrix_ref, updated_ref, whole_ref, coef_ref, hist, block, whole, sides, sems):
    read_hist = pltpu.make_async_copy(hist_ref, hist, sems.at[0])
    read_block = pltpu.make_async_copy(matrix_ref, block, sems.at[1])
    read_hist.start()
    read_block.start()
    coef_ref[...] = u_ref[COEF, 0:2, 0:PANEL_COLUMNS]
    u = [u_ref[m] for m in range(TILES)]
    p, kappa = image_of(got_ref, h_ref, u, u_ref[SCALE, 0:1, 0:1])
    read_hist.wait()
    per = TILES * 8
    for m in range(TILES):
        n = (PANEL_COLUMNS - 1) * per + 8 * m
        hist[0, n : n + 8, :] = u[m]
        hist[1, n : n + 8, :] = p[m] - kappa * u[m]
    for side, n in ((0, own[0]), (1, own[1])):
        z, m0 = n // 2, 6 * (n % 2)
        for t in range(6):
            for half in range(2):
                rows = pl.ds(half * 8 * per + 8 * (m0 + t) + z, 8, stride=per)
                for k in range(2):
                    at = 16 * k + 8 * half
                    sides[side, at : at + 8, LANES * t : LANES * (t + 1)] = hist[k ^ side, rows, :]

    def pieces(x):
        high = x.astype(jnp.bfloat16)
        rest = x - high.astype(jnp.float32)
        mid = rest.astype(jnp.bfloat16)
        return high, mid, (rest - mid.astype(jnp.float32)).astype(jnp.bfloat16)

    lh, lm, ll = pieces(sides[0].T)
    rh, rm, rl = pieces(sides[1])
    left = jnp.concatenate([lh, lh, lm, lm, lh, ll], axis=1)
    right = jnp.concatenate([rh, rm, rh, rm, rl, rh], axis=0)
    read_block.wait()
    writes = []
    step = 256
    for n in range(block.shape[0] // step):
        rows = slice(step * n, step * (n + 1))
        block[rows, :] = block[rows, :] - jnp.dot(left[rows, :], right, preferred_element_type=jnp.float32)
        writes.append(pltpu.make_async_copy(block.at[rows, :], updated_ref.at[rows, :], sems.at[2 + n]))
        writes[-1].start()
    for half in range(2):
        for m in range(TILES):
            for z in range(8):
                s = TILES * z + m
                rows = pl.ds(half * 8 * per + 8 * m + z, 8, stride=per)
                whole[8 * half : 8 * half + 8, LANES * s : LANES * (s + 1)] = hist[0, rows, :]
    write = pltpu.make_async_copy(whole, whole_ref, sems.at[5])
    write.start()
    for w in writes:
        w.wait()
    write.wait()


def per_device(matrix):
    f32 = jnp.float32
    r, c = lax.axis_index("row"), lax.axis_index("col")
    ways = lax.axis_size("col")
    devices = ways * lax.axis_size("row")
    tile_cols = matrix.shape[1]
    own = jnp.stack([r, c])
    rows = lax.all_to_all(
        matrix.reshape(ways, OWN, tile_cols), "col", split_axis=0, concat_axis=0, tiled=True
    )
    top = jnp.where(r == 0, matrix[:2], 0.0)
    for far in (8, 4, 2, 1):
        top = top + lax.ppermute(top, "row", [(n, n + far) for n in range(0, 16, 2 * far)])
    rows, top = lax.optimization_barrier((rows, jnp.broadcast_to(top, (ways, 2, tile_cols))))
    top = lax.all_to_all(top, "col", split_axis=0, concat_axis=0, tiled=True).reshape(2 * ways, tile_cols)

    def exchange(packed):
        return lax.all_to_all(packed, ("row", "col"), split_axis=0, concat_axis=0, tiled=True)

    def shape(*dims):
        return jax.ShapeDtypeStruct(dims, f32)

    vec, ext, packed = shape(TILES, 8, LANES), shape(TILES + 2, 8, LANES), shape(devices, LANES)
    hist = shape(2, PANEL_COLUMNS, TILES, 8, LANES)
    order = TILES * 8 * LANES
    begin = pl.pallas_call(
        begin_body,
        out_shape=(packed, hist),
        in_specs=[VMEM],
        out_specs=(VMEM, ANY),
        scratch_shapes=[
            pltpu.VMEM((192, LANES), f32),
        ],
        name="begin",
    )
    step = pl.pallas_call(
        step_body,
        out_shape=(vec, ext, packed),
        in_specs=[SMEM] + [VMEM] * 5,
        out_specs=(VMEM,) * 3,
        scratch_shapes=[pltpu.VMEM((order // LANES, LANES), f32)],
        name="step",
    )
    history = pl.pallas_call(
        history_body,
        out_shape=(vec, vec, hist),
        in_specs=[SMEM] + [VMEM] * 4 + [ANY],
        out_specs=(VMEM, VMEM, ANY),
        input_output_aliases={5: 2},
        scratch_shapes=[pltpu.VMEM(hist.shape, f32), pltpu.SemaphoreType.DMA((3,))],
        name="history",
    )
    last = pl.pallas_call(
        last_body,
        out_shape=(shape(*matrix.shape), shape(PANEL_COLUMNS, order), shape(2, PANEL_COLUMNS)),
        in_specs=[SMEM] + [VMEM] * 3 + [ANY] * 2,
        out_specs=(ANY, ANY, VMEM),
        scratch_shapes=[
            pltpu.VMEM((2, PANEL_COLUMNS * TILES * 8, LANES), f32),
            pltpu.VMEM(matrix.shape, f32),
            pltpu.VMEM((PANEL_COLUMNS, order), f32),
            pltpu.VMEM((2, 2 * PANEL_COLUMNS, tile_cols), f32),
            pltpu.SemaphoreType.DMA((6,)),
        ],
        name="last",
    )

    def one_column(j, state):
        got, base, h, u, kept = state
        col = jnp.reshape(j, (1,))
        w, un, out = step(col, got, base, h, u, rows)
        got_next = exchange(out)
        base, h, kept = history(col, got, w, u, un, kept)
        return got_next, base, h, un, kept

    def zeros(s):
        return jnp.zeros(s.shape, f32)

    u = jnp.concatenate([zeros(vec), jnp.full((1, 8, LANES), -1.0, f32), jnp.zeros((1, 8, LANES), f32)])
    got, kept = begin(top)
    state = (got, zeros(vec), zeros(vec), u, kept)
    got, _, h, u, kept = lax.fori_loop(0, PANEL_COLUMNS, one_column, state)
    return last(own, got, h, u, kept.reshape(2, -1, LANES), matrix)


def solution(mesh):
    return jax.shard_map(
        per_device,
        mesh=mesh,
        in_specs=(P("row", "col"),),
        out_specs=(P("row", "col"), P(), P()),
        check_vma=False,
    )
```

```python
import functools

import jax
import jax.numpy as jnp
from jax import lax
from jax.experimental import pallas as pl
from jax.experimental.pallas import tpu as pltpu
from jax.sharding import PartitionSpec as P

PANEL_COLUMNS = 16
LANES = 128
TILES = 12
SCALE, COEF = TILES, TILES + 1
OWN = 48

VMEM = pl.BlockSpec(memory_space=pltpu.VMEM)
SMEM = pl.BlockSpec(memory_space=pltpu.SMEM)
HBM = pl.BlockSpec(memory_space=pltpu.HBM)


def total(x):
    return jnp.sum(jnp.sum(x, axis=0, keepdims=True), axis=1, keepdims=True)


def iota(shape, dim):
    return lax.broadcasted_iota(jnp.int32, shape, dim)


def unpack(load):
    lane = iota((8, LANES), 1)
    tiles = []
    for gm in range(4):
        q = [load(8 * gm + k) for k in range(8)]
        tiles.append(jnp.where(lane < 48, q[0], jnp.where(lane < 96, q[1], q[2])))
        tiles.append(jnp.where(lane < 16, q[2], jnp.where(lane < 64, q[3], jnp.where(lane < 112, q[4], q[5]))))
        tiles.append(jnp.where(lane < 32, q[5], jnp.where(lane < 80, q[6], q[7])))
    return tiles


def tree_sum(xs):
    xs = list(xs)
    while len(xs) > 1:
        xs = [xs[i] + xs[i + 1] if i + 1 < len(xs) else xs[i] for i in range(0, len(xs), 2)]
    return xs[0]


def position(m):
    return (iota((8, LANES), 0) * TILES + m) * LANES + iota((8, LANES), 1)


def message(first, second):
    device = lax.axis_index("row") * lax.axis_size("col") + lax.axis_index("col")
    place = iota((OWN, LANES), 1) - iota((OWN, LANES), 0) - OWN * device
    picked = jnp.where((place & (LANES - 1)) == 0, first, 0.0) + jnp.where((place & (LANES - 1)) == OWN, second, 0.0)
    return jnp.sum(picked, axis=0, keepdims=True)


def own_column(rows_ref, k):
    head = rows_ref[0, :, 0:LANES]
    return jnp.sum(jnp.where(iota((OWN, LANES), 1) == k, head, 0.0), axis=1, keepdims=True)


def begin_body(top_ref, out_ref, tmp):
    lane = iota((8, LANES), 1)
    for t in range(6):
        tmp[32 * t : 32 * (t + 1), :] = top_ref[:, LANES * t : LANES * (t + 1)]

    def tile(k, m):
        half, t = divmod(m, 6)
        return tmp[pl.ds(32 * t + 2 * half + k, 8, stride=4), :]

    for gm in range(4):
        rows = []
        for k in range(2):
            t = [tile(k, 3 * gm + n) for n in range(3)]
            rows.append([t[0], t[0], jnp.where(lane < 96, t[1], t[0]), t[1], t[1], jnp.where(lane < 112, t[2], t[1]), t[2], t[2]])
        for q in range(8):
            mine = ((lane - OWN * q) & (LANES - 1)) < OWN
            out_ref[pl.ds(8 * gm + q, 8, stride=32), :] = jnp.where(mine, rows[0][q], pltpu.roll(rows[1][q], OWN, 1))

def image_of(got_ref, h, u, scale):
    y = unpack(lambda first: got_ref[pl.ds(first, 8, stride=32), :])
    p = [scale * (y[m] - h[m]) for m in range(TILES)]
    kappa = 0.5 * scale * total(tree_sum(p[m] * u[m] for m in range(TILES)))
    return p, kappa


def at(x, k):
    return x[0:1, k : k + 1]


def tiles(ref):
    return [ref[m] for m in range(TILES)]


def older_terms(pairs, u, j):
    h = [jnp.zeros((8, LANES), jnp.float32) for _ in range(TILES)]
    base = [jnp.zeros((8, LANES), jnp.float32) for _ in range(TILES)]
    for v_ref, w_ref in pairs:
        v, w = tiles(v_ref), tiles(w_ref)
        vu = total(tree_sum(v[m] * u[m] for m in range(TILES)))
        wu = total(tree_sum(w[m] * u[m] for m in range(TILES)))
        vj, wj = at(v[0], j), at(w[0], j)
        for m in range(TILES):
            h[m] = h[m] + (wu * v[m] + vu * w[m])
            base[m] = base[m] - (wj * v[m] + vj * w[m])
    return h, base


def step_body(j, *refs):
    got_ref, rows_ref = refs[:2]
    un_ref, coming_out, out_ref = refs[-4:-1] if j == 0 else refs[-5:-2]
    flat_ref = refs[-1]
    if j == 0:
        column = unpack(lambda first: got_ref[pl.ds(first, 8, stride=32), :])
        leading = at(column[0], 1)
    else:
        u_ref, coming_ref = refs[2:4]
        w_ref = refs[-2]
        pairs = [(refs[4 + 2 * i], refs[5 + 2 * i]) for i in range(j - 1)]
        u = tiles(u_ref)
        h, base = older_terms(pairs, u, j)
        p, kappa = image_of(got_ref, h, u, u_ref[SCALE, 0:1, 0:1])
        for m in range(TILES):
            base[m] = base[m] + coming_ref[m]
            w_ref[m] = p[m] - kappa * u[m]
        factor = at(p[0], j) - kappa * at(u[0], j) - kappa
        leading = at(base[0], j + 1) - at(p[0], j + 1) - factor * at(u[0], j + 1)
        column = [base[m] - p[m] - factor * u[m] for m in range(TILES)]
    column[0] = jnp.where(position(0) > j, column[0], 0.0)
    for m in range(TILES):
        rest = jnp.where(position(0) == j + 1, 0.0, column[0]) if m == 0 else column[m]
        flat_ref[pl.ds(m, 8, stride=TILES), :] = rest
    norm = jnp.sqrt(total(tree_sum(x * x for x in column)))
    inverse = 1.0 / (leading + norm)
    scale_now = 1.0 + leading / norm

    def four_blocks(n, acc):
        acc = list(acc)
        for s in range(24):
            k, t = divmod(s, 6)
            part = rows_ref[4 * n + k, :, LANES * t : LANES * (t + 1)] * flat_ref[pl.ds(24 * n + s, 1), :]
            acc[s % 2] = acc[s % 2] + part
        return tuple(acc)

    acc = lax.fori_loop(0, 4, four_blocks, (jnp.zeros((OWN, LANES), jnp.float32),) * 2)
    product = jnp.sum(acc[0] + acc[1], axis=1, keepdims=True) * inverse + rows_ref[0, :, j + 1 : j + 2]
    out_ref[...] = jnp.broadcast_to(message(product, rows_ref[0, :, j + 2 : j + 3]), out_ref.shape)
    after = unpack(lambda first: pltpu.roll(got_ref[pl.ds(first, 8, stride=32), :], LANES - OWN, 1))
    for m in range(TILES):
        r = column[m] * inverse
        un_ref[m] = jnp.where(position(0) == j + 1, 1.0, r) if m == 0 else r
        coming_out[m] = after[m]
    un_ref[SCALE] = jnp.broadcast_to(scale_now, (8, LANES))
    lane, row = iota((8, LANES), 1), iota((8, LANES), 0)
    before = jnp.zeros((8, LANES), jnp.float32) if j == 0 else u_ref[COEF]
    un_ref[COEF] = jnp.where(lane == j, jnp.where(row == 0, scale_now, -norm), before)


def last_body(own, got_ref, *refs):
    count = PANEL_COLUMNS - 1
    pairs = [(refs[2 * i], refs[2 * i + 1]) for i in range(count)]
    u_ref, matrix_ref, updated_ref, whole_ref, coef_ref, hist, block, whole, sides, sems = refs[2 * count :]
    read_block = pltpu.make_async_copy(matrix_ref, block, sems.at[0])
    read_block.start()
    coef_ref[...] = u_ref[COEF, 0:2, 0:PANEL_COLUMNS]
    u = tiles(u_ref)
    h, _ = older_terms(pairs, u, 0)
    p, kappa = image_of(got_ref, h, u, u_ref[SCALE, 0:1, 0:1])
    per = TILES * 8
    for i in range(PANEL_COLUMNS):
        for m in range(TILES):
            n = i * per + 8 * m
            hist[0, n : n + 8, :] = pairs[i][0][m] if i < count else u[m]
            hist[1, n : n + 8, :] = pairs[i][1][m] if i < count else p[m] - kappa * u[m]
    for side, n in ((0, own[0]), (1, own[1])):
        z, m0 = n // 2, 6 * (n % 2)
        for t in range(6):
            for half in range(2):
                rows = pl.ds(half * 8 * per + 8 * (m0 + t) + z, 8, stride=per)
                for k in range(2):
                    at = 16 * k + 8 * half
                    sides[side, at : at + 8, LANES * t : LANES * (t + 1)] = hist[k ^ side, rows, :]

    def pieces(x):
        high = x.astype(jnp.bfloat16)
        rest = x - high.astype(jnp.float32)
        mid = rest.astype(jnp.bfloat16)
        return high, mid, (rest - mid.astype(jnp.float32)).astype(jnp.bfloat16)

    lh, lm, ll = pieces(sides[0].T)
    rh, rm, rl = pieces(sides[1])
    left = jnp.concatenate([lh, lh, lm, lm, lh, ll], axis=1)
    right = jnp.concatenate([rh, rm, rh, rm, rl, rh], axis=0)
    read_block.wait()
    writes = []
    step = 256
    for n in range(block.shape[0] // step):
        rows = slice(step * n, step * (n + 1))
        block[rows, :] = block[rows, :] - jnp.dot(left[rows, :], right, preferred_element_type=jnp.float32)
        writes.append(pltpu.make_async_copy(block.at[rows, :], updated_ref.at[rows, :], sems.at[1 + n]))
        writes[-1].start()
    for half in range(2):
        for m in range(TILES):
            for z in range(8):
                s = TILES * z + m
                rows = pl.ds(half * 8 * per + 8 * m + z, 8, stride=per)
                whole[8 * half : 8 * half + 8, LANES * s : LANES * (s + 1)] = hist[0, rows, :]
    write = pltpu.make_async_copy(whole, whole_ref, sems.at[4])
    write.start()
    for w in writes:
        w.wait()
    write.wait()


def per_device(matrix):
    f32 = jnp.float32
    r, c = lax.axis_index("row"), lax.axis_index("col")
    ways = lax.axis_size("col")
    devices = ways * lax.axis_size("row")
    tile_cols = matrix.shape[1]
    own = jnp.stack([r, c])
    top = lax.all_to_all(
        jnp.broadcast_to(matrix[:2], (ways, 2, tile_cols)), "col", split_axis=0, concat_axis=0, tiled=True
    ).reshape(2 * ways, tile_cols)
    top, matrix_after = lax.optimization_barrier((top, matrix))
    top = jnp.where(r == 0, top, 0.0)
    for far in (8, 4, 2, 1):
        top = top + lax.ppermute(top, "row", [(n, n + far) for n in range(0, 16, 2 * far)])
    rows = lax.all_to_all(
        matrix_after.reshape(ways, OWN, tile_cols), "col", split_axis=0, concat_axis=0, tiled=True
    )

    def exchange(packed):
        return lax.all_to_all(packed, ("row", "col"), split_axis=0, concat_axis=0, tiled=True)

    def shape(*dims):
        return jax.ShapeDtypeStruct(dims, f32)

    vec, ext, packed = shape(TILES, 8, LANES), shape(TILES + 2, 8, LANES), shape(devices, LANES)
    order = TILES * 8 * LANES
    begin = pl.pallas_call(
        begin_body,
        out_shape=packed,
        in_specs=[VMEM],
        out_specs=VMEM,
        scratch_shapes=[pltpu.VMEM((192, LANES), f32)],
        compiler_params=pltpu.CompilerParams(vmem_limit_bytes=4 << 20),
        name="begin",
    )

    def step(j, *args):
        out = (ext, vec, packed) + ((vec,) if j else ())
        return pl.pallas_call(
            functools.partial(step_body, j),
            out_shape=out,
            in_specs=[VMEM] * len(args),
            out_specs=(VMEM,) * len(out),
            scratch_shapes=[pltpu.VMEM((order // LANES, LANES), f32)],
            compiler_params=pltpu.CompilerParams(vmem_limit_bytes=8 << 20),
            name=f"step{j}",
        )(*args)

    got, kept, tail = begin(top), [], []
    for j in range(PANEL_COLUMNS):
        u, coming, out, *w = step(j, got, rows, *tail, *kept)
        if j:
            kept += [tail[0], w[0]]
        got, tail = exchange(out), [u, coming]
    last = pl.pallas_call(
        last_body,
        out_shape=(shape(*matrix.shape), shape(PANEL_COLUMNS, order), shape(2, PANEL_COLUMNS)),
        in_specs=[SMEM] + [VMEM] * (len(kept) + 2) + [HBM],
        out_specs=(HBM, HBM, VMEM),
        scratch_shapes=[
            pltpu.VMEM((2, PANEL_COLUMNS * TILES * 8, LANES), f32),
            pltpu.VMEM(matrix.shape, f32),
            pltpu.VMEM((PANEL_COLUMNS, order), f32),
            pltpu.VMEM((2, 2 * PANEL_COLUMNS, tile_cols), f32),
            pltpu.SemaphoreType.DMA((5,)),
        ],
        compiler_params=pltpu.CompilerParams(vmem_limit_bytes=16 << 20),
        name="last",
    )
    return last(own, got, *kept, tail[0], matrix)


def solution(mesh):
    return jax.shard_map(
        per_device,
        mesh=mesh,
        in_specs=(P("row", "col"),),
        out_specs=(P("row", "col"), P(), P()),
        check_vma=False,
    )
```

```python
import functools

import jax
import jax.numpy as jnp
from jax import lax
from jax.experimental import pallas as pl
from jax.experimental.pallas import tpu as pltpu
from jax.sharding import PartitionSpec as P

PANEL_COLUMNS = 16
LANES = 128
TILES = 12
SCALE, COEF = TILES, TILES + 1
OWN = 48

VMEM = pl.BlockSpec(memory_space=pltpu.VMEM)
HBM = pl.BlockSpec(memory_space=pltpu.HBM)


def total(x):
    return jnp.sum(jnp.sum(x, axis=0, keepdims=True), axis=1, keepdims=True)


def iota(shape, dim):
    return lax.broadcasted_iota(jnp.int32, shape, dim)


def unpack(load):
    lane = iota((8, LANES), 1)
    tiles = []
    for gm in range(4):
        q = [load(8 * gm + k) for k in range(8)]
        tiles.append(jnp.where(lane < 48, q[0], jnp.where(lane < 96, q[1], q[2])))
        tiles.append(jnp.where(lane < 16, q[2], jnp.where(lane < 64, q[3], jnp.where(lane < 112, q[4], q[5]))))
        tiles.append(jnp.where(lane < 32, q[5], jnp.where(lane < 80, q[6], q[7])))
    return tiles


def tree_sum(xs):
    xs = list(xs)
    while len(xs) > 1:
        xs = [xs[i] + xs[i + 1] if i + 1 < len(xs) else xs[i] for i in range(0, len(xs), 2)]
    return xs[0]


def position(m):
    return (iota((8, LANES), 0) * TILES + m) * LANES + iota((8, LANES), 1)


def message(first, second):
    device = lax.axis_index("row") * lax.axis_size("col") + lax.axis_index("col")
    place = iota((OWN, LANES), 1) - iota((OWN, LANES), 0) - OWN * device
    picked = jnp.where((place & (LANES - 1)) == 0, first, 0.0) + jnp.where((place & (LANES - 1)) == OWN, second, 0.0)
    return jnp.sum(picked, axis=0, keepdims=True)


def own_column(rows_ref, k):
    head = rows_ref[0, :, 0:LANES]
    return jnp.sum(jnp.where(iota((OWN, LANES), 1) == k, head, 0.0), axis=1, keepdims=True)


def begin_body(top_ref, out_ref, tmp):
    lane = iota((8, LANES), 1)
    for t in range(6):
        tmp[32 * t : 32 * (t + 1), :] = top_ref[:, LANES * t : LANES * (t + 1)]

    def tile(k, m):
        half, t = divmod(m, 6)
        return tmp[pl.ds(32 * t + 2 * half + k, 8, stride=4), :]

    for gm in range(4):
        rows = []
        for k in range(2):
            t = [tile(k, 3 * gm + n) for n in range(3)]
            rows.append([t[0], t[0], jnp.where(lane < 96, t[1], t[0]), t[1], t[1], jnp.where(lane < 112, t[2], t[1]), t[2], t[2]])
        for q in range(8):
            mine = ((lane - OWN * q) & (LANES - 1)) < OWN
            out_ref[pl.ds(8 * gm + q, 8, stride=32), :] = jnp.where(mine, rows[0][q], pltpu.roll(rows[1][q], OWN, 1))

def image_of(got_ref, h, u, scale):
    y = unpack(lambda first: got_ref[pl.ds(first, 8, stride=32), :])
    p = [scale * (y[m] - h[m]) for m in range(TILES)]
    kappa = 0.5 * scale * total(tree_sum(p[m] * u[m] for m in range(TILES)))
    return p, kappa


def at(x, k):
    return x[0:1, k : k + 1]


def tiles(ref):
    return [ref[m] for m in range(TILES)]


def older_terms(pairs, u, j):
    h = [jnp.zeros((8, LANES), jnp.float32) for _ in range(TILES)]
    base = [jnp.zeros((8, LANES), jnp.float32) for _ in range(TILES)]
    for v_ref, w_ref in pairs:
        v, w = tiles(v_ref), tiles(w_ref)
        vu = total(tree_sum(v[m] * u[m] for m in range(TILES)))
        wu = total(tree_sum(w[m] * u[m] for m in range(TILES)))
        vj, wj = at(v[0], j), at(w[0], j)
        for m in range(TILES):
            h[m] = h[m] + (wu * v[m] + vu * w[m])
            base[m] = base[m] - (wj * v[m] + vj * w[m])
    return h, base


def step_body(j, *refs):
    got_ref, rows_ref = refs[:2]
    *outs, flat_ref = refs[-5 if 0 < j < PANEL_COLUMNS - 1 else -4 :]
    un_ref, out_ref = outs[:2]
    if j == 0:
        column = unpack(lambda first: got_ref[pl.ds(first, 8, stride=32), :])
        leading = at(column[0], 1)
    else:
        u_ref, coming_ref = refs[2:4]
        w_ref = outs[-1]
        pairs = [(refs[4 + 2 * i], refs[5 + 2 * i]) for i in range(j - 1)]
        u = tiles(u_ref)
        h, base = older_terms(pairs, u, j)
        p, kappa = image_of(got_ref, h, u, u_ref[SCALE, 0:1, 0:1])
        for m in range(TILES):
            base[m] = base[m] + coming_ref[m]
            w_ref[m] = p[m] - kappa * u[m]
        factor = at(p[0], j) - kappa * at(u[0], j) - kappa
        leading = at(base[0], j + 1) - at(p[0], j + 1) - factor * at(u[0], j + 1)
        column = [base[m] - p[m] - factor * u[m] for m in range(TILES)]
    column[0] = jnp.where(position(0) > j, column[0], 0.0)
    for m in range(TILES):
        rest = jnp.where(position(0) == j + 1, 0.0, column[0]) if m == 0 else column[m]
        flat_ref[pl.ds(m, 8, stride=TILES), :] = rest
    norm = jnp.sqrt(total(tree_sum(x * x for x in column)))
    inverse = 1.0 / (leading + norm)
    scale_now = 1.0 + leading / norm

    def four_blocks(n, acc):
        acc = list(acc)
        for s in range(24):
            k, t = divmod(s, 6)
            part = rows_ref[4 * n + k, :, LANES * t : LANES * (t + 1)] * flat_ref[pl.ds(24 * n + s, 1), :]
            acc[s % 2] = acc[s % 2] + part
        return tuple(acc)

    acc = lax.fori_loop(0, 4, four_blocks, (jnp.zeros((OWN, LANES), jnp.float32),) * 2)
    product = jnp.sum(acc[0] + acc[1], axis=1, keepdims=True) * inverse + rows_ref[0, :, j + 1 : j + 2]
    out_ref[...] = jnp.broadcast_to(message(product, rows_ref[0, :, j + 2 : j + 3]), out_ref.shape)
    for m in range(TILES):
        r = column[m] * inverse
        un_ref[m] = jnp.where(position(0) == j + 1, 1.0, r) if m == 0 else r
    if j < PANEL_COLUMNS - 1:
        after = unpack(lambda first: pltpu.roll(got_ref[pl.ds(first, 8, stride=32), :], LANES - OWN, 1))
        for m in range(TILES):
            outs[2][m] = after[m]
    un_ref[SCALE] = jnp.broadcast_to(scale_now, (8, LANES))
    lane, row = iota((8, LANES), 1), iota((8, LANES), 0)
    before = jnp.zeros((8, LANES), jnp.float32) if j == 0 else u_ref[COEF]
    un_ref[COEF] = jnp.where(lane == j, jnp.where(row == 0, scale_now, -norm), before)


def last_body(got_ref, *refs):
    count = PANEL_COLUMNS - 1
    pairs = [(refs[2 * i], refs[2 * i + 1]) for i in range(count)]
    u_ref, matrix_ref, updated_ref, whole_ref, coef_ref, hist, block, whole, sides, sems = refs[2 * count :]
    coef_ref[...] = u_ref[COEF, 0:2, 0:PANEL_COLUMNS]
    u = tiles(u_ref)
    h, _ = older_terms(pairs, u, 0)
    p, kappa = image_of(got_ref, h, u, u_ref[SCALE, 0:1, 0:1])
    per = TILES * 8
    for i in range(PANEL_COLUMNS):
        for m in range(TILES):
            n = i * per + 8 * m
            hist[0, n : n + 8, :] = pairs[i][0][m] if i < count else u[m]
            hist[1, n : n + 8, :] = pairs[i][1][m] if i < count else p[m] - kappa * u[m]
    for side, n in ((0, lax.axis_index("row")), (1, lax.axis_index("col"))):
        z, m0 = n // 2, 6 * (n % 2)
        for t in range(6):
            for half in range(2):
                rows = pl.ds(half * 8 * per + 8 * (m0 + t) + z, 8, stride=per)
                for k in range(2):
                    at = 16 * k + 8 * half
                    sides[side, at : at + 8, LANES * t : LANES * (t + 1)] = hist[k ^ side, rows, :]

    def pieces(x):
        high = x.astype(jnp.bfloat16)
        rest = x - high.astype(jnp.float32)
        mid = rest.astype(jnp.bfloat16)
        return high, mid, (rest - mid.astype(jnp.float32)).astype(jnp.bfloat16)

    lh, lm, ll = pieces(sides[0].T)
    rh, rm, rl = pieces(sides[1])
    left = jnp.concatenate([lh, lh, lm, lm, lh, ll], axis=1)
    right = jnp.concatenate([rh, rm, rh, rm, rl, rh], axis=0)
    writes = []
    step = 256
    for n in range(block.shape[0] // step):
        rows = slice(step * n, step * (n + 1))
        block[rows, :] = matrix_ref[rows, :] - jnp.dot(left[rows, :], right, preferred_element_type=jnp.float32)
        writes.append(pltpu.make_async_copy(block.at[rows, :], updated_ref.at[rows, :], sems.at[n]))
        writes[-1].start()
    for half in range(2):
        for m in range(TILES):
            for z in range(8):
                s = TILES * z + m
                rows = pl.ds(half * 8 * per + 8 * m + z, 8, stride=per)
                whole[8 * half : 8 * half + 8, LANES * s : LANES * (s + 1)] = hist[0, rows, :]
    write = pltpu.make_async_copy(whole, whole_ref, sems.at[3])
    write.start()
    for w in writes:
        w.wait()
    write.wait()


def per_device(matrix):
    f32 = jnp.float32
    r = lax.axis_index("row")
    ways = lax.axis_size("col")
    devices = ways * lax.axis_size("row")
    tile_cols = matrix.shape[1]
    top = lax.all_to_all(
        jnp.broadcast_to(matrix[:2], (ways, 2, tile_cols)), "col", split_axis=0, concat_axis=0, tiled=True
    ).reshape(2 * ways, tile_cols)
    top, matrix_after = lax.optimization_barrier((top, matrix))
    top = jnp.where(r == 0, top, 0.0)
    for far in (8, 4, 2, 1):
        top = top + lax.ppermute(top, "row", [(n, n + far) for n in range(0, 16, 2 * far)])
    rows = lax.all_to_all(
        matrix_after.reshape(ways, OWN, tile_cols), "col", split_axis=0, concat_axis=0, tiled=True
    )

    def exchange(packed):
        return lax.all_to_all(packed, ("row", "col"), split_axis=0, concat_axis=0, tiled=True)

    def shape(*dims):
        return jax.ShapeDtypeStruct(dims, f32)

    vec, ext, packed = shape(TILES, 8, LANES), shape(TILES + 2, 8, LANES), shape(devices, LANES)
    order = TILES * 8 * LANES
    begin = pl.pallas_call(
        begin_body,
        out_shape=packed,
        in_specs=[VMEM],
        out_specs=VMEM,
        scratch_shapes=[pltpu.VMEM((192, LANES), f32)],
        compiler_params=pltpu.CompilerParams(vmem_limit_bytes=4 << 20),
        name="begin",
    )

    def step(j, *args):
        out = (ext, packed) + (vec,) * ((j < PANEL_COLUMNS - 1) + (j > 0))
        return pl.pallas_call(
            functools.partial(step_body, j),
            out_shape=out,
            in_specs=[VMEM] * len(args),
            out_specs=(VMEM,) * len(out),
            scratch_shapes=[pltpu.VMEM((order // LANES, LANES), f32)],
            compiler_params=pltpu.CompilerParams(vmem_limit_bytes=8 << 20),
            name=f"step{j}",
        )(*args)

    got, kept, tail = begin(top), [], []
    for j in range(PANEL_COLUMNS):
        u, out, *vectors = step(j, got, rows, *tail, *kept)
        if j:
            kept += [tail[0], vectors[-1]]
        got, tail = exchange(out), [u, vectors[0]]
    last = pl.pallas_call(
        last_body,
        out_shape=(shape(*matrix.shape), shape(PANEL_COLUMNS, order), shape(2, PANEL_COLUMNS)),
        in_specs=[VMEM] * (len(kept) + 3),
        out_specs=(HBM, HBM, VMEM),
        scratch_shapes=[
            pltpu.VMEM((2, PANEL_COLUMNS * TILES * 8, LANES), f32),
            pltpu.VMEM(matrix.shape, f32),
            pltpu.VMEM((PANEL_COLUMNS, order), f32),
            pltpu.VMEM((2, 2 * PANEL_COLUMNS, tile_cols), f32),
            pltpu.SemaphoreType.DMA((4,)),
        ],
        compiler_params=pltpu.CompilerParams(vmem_limit_bytes=16 << 20),
        name="last",
    )
    return last(got, *kept, tail[0], matrix)


def solution(mesh):
    return jax.shard_map(
        per_device,
        mesh=mesh,
        in_specs=(P("row", "col"),),
        out_specs=(P("row", "col"), P(), P()),
        check_vma=False,
    )
```

```python
import functools

import jax
import jax.numpy as jnp
from jax import lax
from jax.experimental import pallas as pl
from jax.experimental.pallas import tpu as pltpu
from jax.sharding import PartitionSpec as P

PANEL_COLUMNS = 16
LANES = 128
TILES = 12
SCALE, COEF = TILES, TILES + 1
OWN = 48

VMEM = pl.BlockSpec(memory_space=pltpu.VMEM)
HBM = pl.BlockSpec(memory_space=pltpu.HBM)


def total(x):
    return jnp.sum(jnp.sum(x, axis=0, keepdims=True), axis=1, keepdims=True)


def iota(shape, dim):
    return lax.broadcasted_iota(jnp.int32, shape, dim)


def unpack(load, turn=0):
    lane = (iota((8, LANES), 1) - turn) & (LANES - 1)
    tiles = []
    for gm in range(4):
        q = [load(8 * gm + k) for k in range(8)]
        tiles.append(jnp.where(lane < 48, q[0], jnp.where(lane < 96, q[1], q[2])))
        tiles.append(jnp.where(lane < 16, q[2], jnp.where(lane < 64, q[3], jnp.where(lane < 112, q[4], q[5]))))
        tiles.append(jnp.where(lane < 32, q[5], jnp.where(lane < 80, q[6], q[7])))
    return tiles


def tree_sum(xs):
    xs = list(xs)
    while len(xs) > 1:
        xs = [xs[i] + xs[i + 1] if i + 1 < len(xs) else xs[i] for i in range(0, len(xs), 2)]
    return xs[0]


def position(m):
    return (iota((8, LANES), 0) * TILES + m) * LANES + iota((8, LANES), 1)


def message(first, second):
    device = lax.axis_index("row") * lax.axis_size("col") + lax.axis_index("col")
    place = iota((OWN, LANES), 1) - iota((OWN, LANES), 0) - OWN * device
    picked = jnp.where((place & (LANES - 1)) == 0, first, 0.0) + jnp.where((place & (LANES - 1)) == OWN, second, 0.0)
    return jnp.sum(picked, axis=0, keepdims=True)


def own_column(rows_ref, k):
    head = rows_ref[0, :, 0:LANES]
    return jnp.sum(jnp.where(iota((OWN, LANES), 1) == k, head, 0.0), axis=1, keepdims=True)


def begin_body(top_ref, out_ref, tmp):
    lane = iota((8, LANES), 1)
    for t in range(6):
        tmp[32 * t : 32 * (t + 1), :] = top_ref[:, LANES * t : LANES * (t + 1)]

    def tile(k, m):
        half, t = divmod(m, 6)
        return tmp[pl.ds(32 * t + 2 * half + k, 8, stride=4), :]

    for gm in range(4):
        rows = []
        for k in range(2):
            t = [tile(k, 3 * gm + n) for n in range(3)]
            rows.append([t[0], t[0], jnp.where(lane < 96, t[1], t[0]), t[1], t[1], jnp.where(lane < 112, t[2], t[1]), t[2], t[2]])
        for q in range(8):
            mine = ((lane - OWN * q) & (LANES - 1)) < OWN
            out_ref[pl.ds(8 * gm + q, 8, stride=32), :] = jnp.where(mine, rows[0][q], pltpu.roll(rows[1][q], OWN, 1))

def image_of(got_ref, h, u, scale):
    y = unpack(lambda first: got_ref[pl.ds(first, 8, stride=32), :])
    p = [scale * (y[m] - h[m]) for m in range(TILES)]
    kappa = 0.5 * scale * total(tree_sum(p[m] * u[m] for m in range(TILES)))
    return p, kappa


def at(x, k):
    return x[0:1, k : k + 1]


def tiles(ref):
    return [ref[m] for m in range(TILES)]


def older_terms(pairs, u, j):
    h = [jnp.zeros((8, LANES), jnp.float32) for _ in range(TILES)]
    base = [jnp.zeros((8, LANES), jnp.float32) for _ in range(TILES)]
    for v_ref, w_ref in pairs:
        v, w = tiles(v_ref), tiles(w_ref)
        vu = total(tree_sum(v[m] * u[m] for m in range(TILES)))
        wu = total(tree_sum(w[m] * u[m] for m in range(TILES)))
        vj, wj = at(v[0], j), at(w[0], j)
        for m in range(TILES):
            h[m] = h[m] + (wu * v[m] + vu * w[m])
            base[m] = base[m] - (wj * v[m] + vj * w[m])
    return h, base


def step_body(j, *refs):
    got_ref, rows_ref = refs[:2]
    *outs, flat_ref = refs[-5 if 0 < j < PANEL_COLUMNS - 1 else -4 :]
    un_ref, out_ref = outs[:2]
    if j == 0:
        column = unpack(lambda first: got_ref[pl.ds(first, 8, stride=32), :])
        leading = at(column[0], 1)
    else:
        u_ref, coming_ref = refs[2:4]
        w_ref = outs[-1]
        pairs = [(refs[4 + 2 * i], refs[5 + 2 * i]) for i in range(j - 1)]
        u = tiles(u_ref)
        h, base = older_terms(pairs, u, j)
        p, kappa = image_of(got_ref, h, u, u_ref[SCALE, 0:1, 0:1])
        for m in range(TILES):
            base[m] = base[m] + coming_ref[m]
            w_ref[m] = p[m] - kappa * u[m]
        factor = at(p[0], j) - kappa * at(u[0], j) - kappa
        leading = at(base[0], j + 1) - at(p[0], j + 1) - factor * at(u[0], j + 1)
        column = [base[m] - p[m] - factor * u[m] for m in range(TILES)]
    column[0] = jnp.where(position(0) > j, column[0], 0.0)
    for m in range(TILES):
        rest = jnp.where(position(0) == j + 1, 0.0, column[0]) if m == 0 else column[m]
        flat_ref[pl.ds(m, 8, stride=TILES), :] = rest
    norm = jnp.sqrt(total(tree_sum(x * x for x in column)))
    inverse = 1.0 / (leading + norm)
    scale_now = 1.0 + leading / norm

    def four_blocks(n, acc):
        acc = list(acc)
        for s in range(24):
            k, t = divmod(s, 6)
            part = rows_ref[4 * n + k, :, LANES * t : LANES * (t + 1)] * flat_ref[pl.ds(24 * n + s, 1), :]
            acc[s % 2] = acc[s % 2] + part
        return tuple(acc)

    acc = lax.fori_loop(0, 4, four_blocks, (jnp.zeros((OWN, LANES), jnp.float32),) * 2)
    product = jnp.sum(acc[0] + acc[1], axis=1, keepdims=True) * inverse + rows_ref[0, :, j + 1 : j + 2]
    out_ref[...] = jnp.broadcast_to(message(product, rows_ref[0, :, j + 2 : j + 3]), out_ref.shape)
    for m in range(TILES):
        r = column[m] * inverse
        un_ref[m] = jnp.where(position(0) == j + 1, 1.0, r) if m == 0 else r
    if j < PANEL_COLUMNS - 1:
        after = unpack(lambda first: got_ref[pl.ds(first, 8, stride=32), :], OWN)
        for m in range(TILES):
            outs[2][m] = pltpu.roll(after[m], LANES - OWN, 1)
    un_ref[SCALE] = jnp.broadcast_to(scale_now, (8, LANES))
    lane, row = iota((8, LANES), 1), iota((8, LANES), 0)
    before = jnp.zeros((8, LANES), jnp.float32) if j == 0 else u_ref[COEF]
    un_ref[COEF] = jnp.where(lane == j, jnp.where(row == 0, scale_now, -norm), before)


def last_body(got_ref, *refs):
    count = PANEL_COLUMNS - 1
    pairs = [(refs[2 * i], refs[2 * i + 1]) for i in range(count)]
    u_ref, matrix_ref, updated_ref, whole_ref, coef_ref, hist, block, whole, sides, sems = refs[2 * count :]
    coef_ref[...] = u_ref[COEF, 0:2, 0:PANEL_COLUMNS]
    u = tiles(u_ref)
    h, _ = older_terms(pairs, u, 0)
    p, kappa = image_of(got_ref, h, u, u_ref[SCALE, 0:1, 0:1])
    per = TILES * 8
    for i in range(PANEL_COLUMNS):
        for m in range(TILES):
            n = i * per + 8 * m
            hist[0, n : n + 8, :] = pairs[i][0][m] if i < count else u[m]
            hist[1, n : n + 8, :] = pairs[i][1][m] if i < count else p[m] - kappa * u[m]
    for side, n in ((0, lax.axis_index("row")), (1, lax.axis_index("col"))):
        z, m0 = n // 2, 6 * (n % 2)
        for t in range(6):
            for half in range(2):
                rows = pl.ds(half * 8 * per + 8 * (m0 + t) + z, 8, stride=per)
                for k in range(2):
                    at = 16 * k + 8 * half
                    sides[side, at : at + 8, LANES * t : LANES * (t + 1)] = hist[k ^ side, rows, :]

    def pieces(x):
        high = x.astype(jnp.bfloat16)
        rest = x - high.astype(jnp.float32)
        mid = rest.astype(jnp.bfloat16)
        return high, mid, (rest - mid.astype(jnp.float32)).astype(jnp.bfloat16)

    lh, lm, ll = pieces(sides[0].T)
    rh, rm, rl = pieces(sides[1])
    left = jnp.concatenate([lh, lh, lm, lm, lh, ll], axis=1)
    right = jnp.concatenate([rh, rm, rh, rm, rl, rh], axis=0)
    writes = []
    step = 256
    for n in range(block.shape[0] // step):
        rows = slice(step * n, step * (n + 1))
        block[rows, :] = matrix_ref[rows, :] - jnp.dot(left[rows, :], right, preferred_element_type=jnp.float32)
        writes.append(pltpu.make_async_copy(block.at[rows, :], updated_ref.at[rows, :], sems.at[n]))
        writes[-1].start()
    for half in range(2):
        for m in range(TILES):
            for z in range(8):
                s = TILES * z + m
                rows = pl.ds(half * 8 * per + 8 * m + z, 8, stride=per)
                whole[8 * half : 8 * half + 8, LANES * s : LANES * (s + 1)] = hist[0, rows, :]
    write = pltpu.make_async_copy(whole, whole_ref, sems.at[3])
    write.start()
    for w in writes:
        w.wait()
    write.wait()


def per_device(matrix):
    f32 = jnp.float32
    r = lax.axis_index("row")
    ways = lax.axis_size("col")
    devices = ways * lax.axis_size("row")
    tile_cols = matrix.shape[1]
    top = lax.all_to_all(
        jnp.broadcast_to(matrix[:2], (ways, 2, tile_cols)), "col", split_axis=0, concat_axis=0, tiled=True
    ).reshape(2 * ways, tile_cols)
    top, matrix_after = lax.optimization_barrier((top, matrix))
    top = jnp.where(r == 0, top, 0.0)
    for far in (8, 4, 2, 1):
        top = top + lax.ppermute(top, "row", [(n, n + far) for n in range(0, 16, 2 * far)])
    rows = lax.all_to_all(
        matrix_after.reshape(ways, OWN, tile_cols), "col", split_axis=0, concat_axis=0, tiled=True
    )

    def exchange(packed):
        return lax.all_to_all(packed, ("row", "col"), split_axis=0, concat_axis=0, tiled=True)

    def shape(*dims):
        return jax.ShapeDtypeStruct(dims, f32)

    vec, ext, packed = shape(TILES, 8, LANES), shape(TILES + 2, 8, LANES), shape(devices, LANES)
    order = TILES * 8 * LANES
    begin = pl.pallas_call(
        begin_body,
        out_shape=packed,
        in_specs=[VMEM],
        out_specs=VMEM,
        scratch_shapes=[pltpu.VMEM((192, LANES), f32)],
        compiler_params=pltpu.CompilerParams(vmem_limit_bytes=4 << 20),
        name="begin",
    )

    def step(j, *args):
        out = (ext, packed) + (vec,) * ((j < PANEL_COLUMNS - 1) + (j > 0))
        return pl.pallas_call(
            functools.partial(step_body, j),
            out_shape=out,
            in_specs=[VMEM] * len(args),
            out_specs=(VMEM,) * len(out),
            scratch_shapes=[pltpu.VMEM((order // LANES, LANES), f32)],
            compiler_params=pltpu.CompilerParams(vmem_limit_bytes=8 << 20),
            name=f"step{j}",
        )(*args)

    got, kept, tail = begin(top), [], []
    for j in range(PANEL_COLUMNS):
        u, out, *vectors = step(j, got, rows, *tail, *kept)
        if j:
            kept += [tail[0], vectors[-1]]
        got, tail = exchange(out), [u, vectors[0]]
    last = pl.pallas_call(
        last_body,
        out_shape=(shape(*matrix.shape), shape(PANEL_COLUMNS, order), shape(2, PANEL_COLUMNS)),
        in_specs=[VMEM] * (len(kept) + 3),
        out_specs=(HBM, HBM, VMEM),
        scratch_shapes=[
            pltpu.VMEM((2, PANEL_COLUMNS * TILES * 8, LANES), f32),
            pltpu.VMEM(matrix.shape, f32),
            pltpu.VMEM((PANEL_COLUMNS, order), f32),
            pltpu.VMEM((2, 2 * PANEL_COLUMNS, tile_cols), f32),
            pltpu.SemaphoreType.DMA((4,)),
        ],
        compiler_params=pltpu.CompilerParams(vmem_limit_bytes=16 << 20),
        name="last",
    )
    return last(got, *kept, tail[0], matrix)


def solution(mesh):
    return jax.shard_map(
        per_device,
        mesh=mesh,
        in_specs=(P("row", "col"),),
        out_specs=(P("row", "col"), P(), P()),
        check_vma=False,
    )
```
